32 devices in a mesh: grp: 2 (over x), wide: 16 (over z, y, core).
Axes of the slice: x: 2, y: 2, z: 4, core: 2. Of those that a mesh axis runs over, the one named last changes fastest.
Arguments:
- x_pool: bfloat16 [16384, 7168], P(('grp', 'wide')), may hold values from -6 to 6
- token_ids: int32 [4096], P(('grp', 'wide')), may hold values from 0 to 16383, as said below
- cotangent: bfloat16 [4096, 7168], P(('grp', 'wide')), may hold values from -6 to 6
- gate_up: bfloat16 [2, 1024, 7168], P(None, 'wide', 'grp'), may hold values from -0.0625 to 0.0625
- down_weight: bfloat16 [1024, 7168], P('wide', 'grp'), may hold values from -0.1875 to 0.1875
- loss_exponent: int32 [1], replicated, may hold values from 3 to 9
Outputs:
- grad_gate_up: bfloat16 [2, 1024, 7168], P(None, 'wide', 'grp')
- grad_down: bfloat16 [1024, 7168], P('wide', 'grp')
The draws below stay inside these ranges and needn't reach their ends.
Inputs may be any that keep to these rules, and one draw needn't show every extreme that they name: The 128 ids in aligned block b of token_ids name rows b * 512 to (b + 1) * 512 - 1 of x_pool.
All inputs are finite; a program needn't handle non-finite values.
Results may differ from the reference program's by a relative error of at most 0.014.
Values may be sent and summed in bfloat16 or wider, within the bound.
A program may use at most 192 MiB of HBM per device.

```python
import jax
import jax.numpy as jnp
import numpy as np

D = 7168
F = 1024
BLOCKS = 8
TOK_DEV = 128
POOL_DEV = 512
TOKENS = 4096
POOL = 16384
N_GRP = 2
N_WIDE = 16


def draw_token_ids(key, part):
    offsets = jnp.arange(TOKENS, dtype=jnp.int32) // TOK_DEV * POOL_DEV
    return offsets + jax.random.randint(key, (TOKENS,), 0, POOL_DEV, dtype=jnp.int32)


def shard_levels(key, shape, pieces, smallest, top_value):
    level, own = 1.0, jax.random.fold_in(key, 6)
    for dim, shards_of in pieces:
        heights = jnp.exp(jax.random.uniform(jax.random.fold_in(own, dim), (shards_of,), jnp.float32, smallest / len(pieces), top_value / len(pieces)))
        level = level * jnp.repeat(heights, shape[dim] // shards_of).reshape([-1 if axis == dim else 1 for axis in range(len(shape))])
    return level


def scatter_about(key, extent, width, limit, cuts=(), held_as=jnp.bfloat16):
    gain = shard_levels(key, extent, cuts, -0.22, 0.18) if cuts else 1.0
    drawn = jax.random.normal(key, extent, jnp.float32) * width * gain
    return jnp.minimum(jnp.maximum(drawn, -limit), limit).astype(held_as)


def setup_inputs(seed: int = 0) -> dict:
    key_of = jax.random.split(jax.random.key(seed), 7)
    return {
        "x_pool": scatter_about(key_of[0], (POOL, D), 1.0, 6.0, ((0, 32),)),
        "token_ids": draw_token_ids(jax.random.fold_in(key_of[6], 71), 0),
        "cotangent": scatter_about(key_of[2], (TOKENS, D), 1.0, 6.0, ((0, 32),)),
        "gate_up": scatter_about(key_of[3], (2, F, D), D ** -0.5, 0.0625, ((1, 16), (2, 2))),
        "down_weight": scatter_about(key_of[4], (F, D), F ** -0.5, 0.1875, ((0, 16), (1, 2))),
        "loss_exponent": jax.random.randint(key_of[5], (1,), 3, 10).astype(jnp.int32),
    }


def unscale_of(loss_exponent):
    levels = jnp.arange(16, dtype=jnp.int32)
    powers = jnp.asarray(np.power(0.5, np.arange(16)), dtype=jnp.float32)
    return jnp.sum(jnp.where(levels == loss_exponent[0], powers, jnp.float32(0.0)))


def reference(x_pool, token_ids, cotangent, gate_up, down_weight, loss_exponent):
    picked = jnp.take(x_pool, token_ids, axis=0)
    unscale = unscale_of(loss_exponent)
    gate_act = jnp.dot(picked, gate_up[0].T, preferred_element_type=jnp.float32)
    up_act = jnp.dot(picked, gate_up[1].T, preferred_element_type=jnp.float32)
    delta_hidden = unscale * jnp.dot(cotangent, down_weight.T, preferred_element_type=jnp.float32)
    sigmoid_gate = jax.nn.sigmoid(gate_act)
    hidden = (gate_act * sigmoid_gate * up_act).astype(jnp.bfloat16)
    delta_gate = (delta_hidden * up_act * sigmoid_gate * (1.0 + gate_act * (1.0 - sigmoid_gate))).astype(jnp.bfloat16)
    delta_up = (delta_hidden * gate_act * sigmoid_gate).astype(jnp.bfloat16)
    set_count = N_GRP * (N_WIDE // BLOCKS)
    set_rows = TOKENS // set_count
    total_gate = jnp.zeros((F, D), jnp.float32)
    total_up = jnp.zeros((F, D), jnp.float32)
    total_down = jnp.zeros((F, D), jnp.float32)
    for set_index in range(set_count):
        lower = set_index * set_rows
        upper = lower + set_rows
        rows_in = picked[lower:upper]
        part_gate = jnp.dot(delta_gate[lower:upper].T, rows_in, preferred_element_type=jnp.float32)
        part_up = jnp.dot(delta_up[lower:upper].T, rows_in, preferred_element_type=jnp.float32)
        part_down = unscale * jnp.dot(hidden[lower:upper].T, cotangent[lower:upper], preferred_element_type=jnp.float32)
        total_gate = total_gate + part_gate.astype(jnp.bfloat16).astype(jnp.float32)
        total_up = total_up + part_up.astype(jnp.bfloat16).astype(jnp.float32)
        total_down = total_down + part_down.astype(jnp.bfloat16).astype(jnp.float32)
    grad_gate_up = jnp.stack([total_gate, total_up]).astype(jnp.bfloat16)
    grad_down = total_down.astype(jnp.bfloat16)
    return grad_gate_up, grad_down
```

```python
import jax
import jax.numpy as jnp
import numpy as np
from jax import lax
from jax.sharding import PartitionSpec as P


def unscale_of(loss_exponent):
    levels = jnp.arange(16, dtype=jnp.int32)
    powers = jnp.asarray(np.power(0.5, np.arange(16)), dtype=jnp.float32)
    return jnp.sum(jnp.where(levels == loss_exponent[0], powers, jnp.float32(0.0)))


def contract_last(left_side, right_side):
    return lax.dot_general(
        left_side, right_side, (((1,), (1,)), ((), ())), preferred_element_type=jnp.float32
    )


def matmul(left_side, right_side):
    return lax.dot_general(
        left_side, right_side, (((1,), (0,)), ((), ())), preferred_element_type=jnp.float32
    )


def swapped(value, axis, bit):
    mask = 2**bit
    pairs = [(source, source ^ mask) for source in range(lax.axis_size(axis))]
    return lax.ppermute(value, axis, pairs)


def gather_near(value, bits):
    pieces = [value]
    for bit in reversed(range(bits)):
        pieces = pieces + [swapped(piece, "wide", bit) for piece in pieces]
    return jnp.concatenate(pieces, axis=0)


def line_pairs(rows, near, step, reach):
    pairs = []
    for row in range(rows):
        origin = row - step * reach
        target = row + step
        if 0 <= origin < rows and 0 <= target < rows:
            pairs += [(row * near + slot, target * near + slot) for slot in range(near)]
    return pairs


def per_device(x_pool, token_ids, cotangent, gate_up, down_weight, loss_exponent):
    wide_count = lax.axis_size("wide")
    bits = wide_count.bit_length() - 1
    near_bits = bits - bits // 2
    near = 2**near_bits
    rows = wide_count // near
    grp = lax.axis_index("grp")
    wide_index = lax.axis_index("wide")
    row = wide_index // near
    half = gate_up.shape[2]
    units = gate_up.shape[1]
    device_index = grp * wide_count + wide_index
    unscale = unscale_of(loss_exponent)

    tile = jnp.concatenate([gate_up, down_weight[None]], axis=0)
    from_left, from_right = [tile], [tile]
    for reach in range(rows - 1):
        from_left.append(lax.ppermute(from_left[-1], "wide", line_pairs(rows, near, 1, reach)))
        from_right.append(lax.ppermute(from_right[-1], "wide", line_pairs(rows, near, -1, reach)))
    slots = [tile]
    for slot in range(1, rows):
        slots.append(jnp.where(row + slot < rows, from_right[slot], from_left[rows - slot]))
    weights = [jnp.concatenate([slot[kind] for slot in slots], axis=0) for kind in range(3)]

    local_rows = token_ids - device_index * x_pool.shape[0]
    pool_rows = lax.broadcasted_iota(jnp.int32, (token_ids.shape[0], x_pool.shape[0]), 1)
    pick = (local_rows[:, None] == pool_rows).astype(jnp.bfloat16)

    def feature_half(which):
        pool_half = lax.dynamic_slice_in_dim(x_pool, which * half, half, axis=1)
        grad_half = lax.dynamic_slice_in_dim(cotangent, which * half, half, axis=1)
        return matmul(pick, pool_half).astype(jnp.bfloat16), grad_half

    other_in, other_grad = feature_half(1 - grp)
    far_in = swapped(other_in, "grp", 0)
    far_grad = swapped(other_grad, "grp", 0)
    own_in, own_grad = feature_half(grp)
    tokens_in = [gather_near(own_in, near_bits), gather_near(far_in, near_bits)]
    tokens_grad = [gather_near(own_grad, near_bits), gather_near(far_grad, near_bits)]

    def project(weight, tokens):
        return [contract_last(weight, part) for part in tokens]

    partial = [
        project(weights[0], tokens_in),
        project(weights[1], tokens_in),
        project(weights[2], tokens_grad),
    ]
    totals = []
    for own_half, far_half in partial:
        sent = jnp.concatenate([far_half, own_half], axis=1).astype(jnp.bfloat16)
        arrived = swapped(sent, "grp", 0).astype(jnp.float32)
        totals.append(jnp.concatenate([own_half, far_half], axis=1) + arrived)
    gate_act, up_act, delta_hidden = totals
    delta_hidden = unscale * delta_hidden
    sigmoid_gate = jax.nn.sigmoid(gate_act)
    hidden = (gate_act * sigmoid_gate * up_act).astype(jnp.bfloat16)
    delta_gate = (
        delta_hidden * up_act * sigmoid_gate * (1.0 + gate_act * (1.0 - sigmoid_gate))
    ).astype(jnp.bfloat16)
    delta_up = (delta_hidden * gate_act * sigmoid_gate).astype(jnp.bfloat16)

    def gradient(delta, tokens):
        split = tokens[0].shape[0]
        return matmul(delta[:, :split], tokens[0]) + matmul(delta[:, split:], tokens[1])

    grads = [
        gradient(delta_gate, tokens_in).astype(jnp.bfloat16),
        gradient(delta_up, tokens_in).astype(jnp.bfloat16),
        (unscale * gradient(hidden, tokens_grad)).astype(jnp.bfloat16),
    ]

    def part_of(slot):
        return jnp.stack([grad[slot * units : (slot + 1) * units] for grad in grads])

    right_in = left_in = None
    for reach in reversed(range(1, rows)):
        right_out, left_out = part_of(reach), part_of(rows - reach)
        if right_in is not None:
            right_out = (right_out.astype(jnp.float32) + right_in.astype(jnp.float32)).astype(jnp.bfloat16)
            left_out = (left_out.astype(jnp.float32) + left_in.astype(jnp.float32)).astype(jnp.bfloat16)
        right_pairs = [
            (r * near + s, (r + 1) * near + s) for r in range(rows - reach) for s in range(near)
        ]
        last = rows - 1
        left_pairs = [
            ((last - s // near) * near + s % near, (last - t // near) * near + t % near)
            for s, t in right_pairs
        ]
        right_in = lax.ppermute(right_out, "wide", right_pairs)
        left_in = lax.ppermute(left_out, "wide", left_pairs)
    finished = (
        part_of(0).astype(jnp.float32) + right_in.astype(jnp.float32) + left_in.astype(jnp.float32)
    ).astype(jnp.bfloat16)
    return (finished[:2], finished[2])


def solution(mesh):
    in_specs = (
        P(("grp", "wide"), None),
        P(("grp", "wide")),
        P(("grp", "wide"), None),
        P(None, "wide", "grp"),
        P("wide", "grp"),
        P(),
    )
    out_specs = (P(None, "wide", "grp"), P("wide", "grp"))
    return jax.shard_map(
        per_device, mesh=mesh, in_specs=in_specs, out_specs=out_specs, check_vma=False
    )
```
